32 devices in a mesh: grp: 4 (over z), blk: 8 (over y, x, core).
Axes of the slice: x: 2, y: 2, z: 4, core: 2. Of those that a mesh axis runs over, the one named last changes fastest.
Arguments:
- node_features: bfloat16 [40960, 256], P(('grp', 'blk')), may hold values from -6 to 6
- norm_gain: float32 [256], replicated, may hold values from 0.1 to 1.9
- norm_shift: float32 [256], replicated, may hold values from -4 to 4
- query_weight: bfloat16 [256, 256], replicated, may hold values from -16 to 16
- key_value_weight: bfloat16 [256, 512], replicated, may hold values from -0.375 to 0.375
- out_weight: bfloat16 [256, 256], replicated, may hold values from -1 to 1
- up_weight: bfloat16 [256, 1024], replicated, may hold values from -0.375 to 0.375
- down_weight: bfloat16 [1024, 256], replicated, may hold values from -0.1875 to 0.1875
- neighbour_tiles: int32 [320, 32], P(('grp', 'blk')), may hold values from 0 to 319, as said below
- neighbour_counts: int32 [320], P(('grp', 'blk')), may hold values from 10 to 30, as said below
Outputs:
- updated: bfloat16 [40960, 256], P(('grp', 'blk'))
The draws below stay inside these ranges and needn't reach their ends.
Inputs may be any that keep to these rules, and one draw needn't show every extreme that they name: `neighbour_tiles`: tile id i is held by the device at index i // 10 of grp+blk (grp slowest), as its tile i % 10. Within a group, the device at index b of blk sits at row b // 4 and column b % 4 of a grid with 4 columns; its grid neighbours are the devices of the group whose row and column each differ from its own by at most one. Every entry of row t names a tile of the device of tile t or of one of its grid neighbours; entry 0 is t itself; the valid entries of a row (index below neighbour_counts) are distinct; entries at or after neighbour_counts[t] equal t. The valid entries of one device's rows name exactly 4 distinct tiles of each of its grid neighbours. `neighbour_counts`: at most min(32, 10 + 4 times the number of grid neighbours of the tile's device); this most is reached on the device at grid row 1, column 1 of every group.
All inputs are finite; a program needn't handle non-finite values. Where the reference program divides by a largest or mean magnitude, that divisor is 1e-20 or more.
Results may differ from the reference program's by a relative error of at most 0.011.
Values may be sent and summed in bfloat16 or wider, within the bound.
A program may use at most 64 MiB of HBM per device.

```python
import math
import jax
import jax.numpy as jnp
from jax import lax

D = 256
HEADS = 8
FF = 1024
TILE = 128
NB = 32
GW = 4
CAP = 4
MINC = 10
TPD = 10
TILES = 320
NODES = 40960
N_GRP = 4
N_BLK = 8


def key_value_base(key):
    sample = jax.random.normal(jax.random.fold_in(key, 101), (D, 2 * D), jnp.float32)
    return jnp.clip(sample, -6.0, 6.0) / jnp.sqrt(jnp.float32(D))


def draw_key_value_weight(key, part):
    return key_value_base(key).astype(jnp.bfloat16)


def draw_query_weight(key, part):
    sample = jax.random.normal(jax.random.fold_in(key, 102), (D, D), jnp.float32)
    noise = jnp.clip(sample, -6.0, 6.0) / jnp.sqrt(jnp.float32(D))
    result = 2.5 * noise
    return result.astype(jnp.bfloat16)


def pick_tiles(subkey):
    return jax.random.permutation(subkey, TPD)[:CAP].astype(jnp.int32)


def neighbour_tables(key):
    base_key = jax.random.fold_in(key, 303)
    row_step = jnp.array([-1, -1, -1, 0, 0, 1, 1, 1], jnp.int32)
    col_step = jnp.array([-1, 0, 1, -1, 1, -1, 0, 1], jnp.int32)
    grid_rows = N_BLK // GW

    def one_device(device):
        device_key = jax.random.fold_in(base_key, device)
        first_key, second_key, third_key, fourth_key = jax.random.split(device_key, 4)
        group_start = device // N_BLK * N_BLK * TPD
        within = device % N_BLK
        my_row = within // GW
        my_col = within % GW
        other_row = my_row + row_step
        other_col = my_col + col_step
        usable = (other_row >= 0) & (other_row < grid_rows) & (other_col >= 0) & (other_col < GW)
        others = jnp.where(usable, other_row * GW + other_col, 0).astype(jnp.int32)
        picks = jax.vmap(pick_tiles)(jax.random.split(first_key, 8))
        remote = (others[:, None] * TPD + picks).reshape(-1)
        unused = jnp.repeat(1 - usable.astype(jnp.int32), CAP)
        shuffle = jax.random.permutation(second_key, 8 * CAP)
        remote = remote[shuffle]
        unused = unused[shuffle]
        order = jnp.argsort(unused, stable=True)
        remote = remote[order]
        spread = CAP * jnp.sum(usable.astype(jnp.int32))
        longest = jnp.minimum(NB, TPD + spread)
        rows = jnp.arange(TPD, dtype=jnp.int32)[:, None]
        places = jnp.arange(NB, dtype=jnp.int32)[None, :]
        remote_pick = remote[(rows * (MINC - 1) + places - 1 + spread) % spread]
        own_pick = within * TPD + (rows + places - spread + TPD * NB) % TPD
        own_tile = within * TPD + rows
        listed = jnp.where(places == 0, own_tile, jnp.where(places <= spread, remote_pick, own_pick))
        upper = jax.random.randint(third_key, (), 12, longest + 1)
        upper = jnp.where(within == GW + 1, longest, upper)
        lengths = jax.random.randint(fourth_key, (TPD,), MINC, upper + 1)
        lengths = lengths.at[0].set(upper)
        listed = jnp.where(places < lengths[:, None], listed, own_tile)
        return ((listed + group_start).astype(jnp.int32), lengths.astype(jnp.int32))
    return jax.vmap(one_device)(jnp.arange(N_GRP * N_BLK, dtype=jnp.int32))


def draw_neighbour_tiles(key, part):
    listed, lengths = neighbour_tables(key)
    return listed.reshape(TILES, NB)


def draw_neighbour_counts(key, part):
    listed, lengths = neighbour_tables(key)
    return lengths.reshape(TILES)


def levels(own_key, dims, cuts, smallest, top_value):
    def one(axis_at, parts):
        draws = jax.random.uniform(jax.random.fold_in(jax.random.fold_in(own_key, 6), axis_at), (parts,), jnp.float32, smallest / len(cuts), top_value / len(cuts))
        return jnp.repeat(jnp.exp(draws), dims[axis_at] // parts).reshape((-1,) + (1,) * (len(dims) - axis_at - 1))

    level = one(*cuts[0])
    for cut in cuts[1:]:
        level = level * one(*cut)
    return level


def bell_draw(key, extent, scale, bound, pieces=(), held_as=jnp.bfloat16):
    entries = jax.random.normal(key, extent, jnp.float32) * scale
    if len(pieces) > 0:
        entries = levels(key, extent, pieces, -0.22, 0.18) * entries
    return jnp.clip(entries, min=-bound, max=bound).astype(held_as)


def setup_inputs(seed: int = 0) -> dict:
    key_list = jax.random.split(jax.random.key(seed), 11)
    node_features = bell_draw(key_list[0], (NODES, D), 1.0, 6.0, ((0, 32),))
    norm_gain = jnp.clip(1.0 + 0.18 * jax.random.normal(key_list[1], (D,), jnp.float32), 0.1, 1.9)
    norm_shift = bell_draw(key_list[2], (D,), 1.0, 4.0, (), jnp.float32)
    query_weight = draw_query_weight(jax.random.fold_in(key_list[10], 71), 0)
    key_value_weight = draw_key_value_weight(jax.random.fold_in(key_list[10], 71), 0)
    out_weight = bell_draw(key_list[5], (D, D), (D // 8) ** -0.5, 1.0)
    up_weight = bell_draw(key_list[6], (D, FF), D ** -0.5, 0.375)
    down_weight = bell_draw(key_list[7], (FF, D), FF ** -0.5, 0.1875)
    neighbour_tiles = draw_neighbour_tiles(jax.random.fold_in(key_list[10], 71), 0)
    neighbour_counts = draw_neighbour_counts(jax.random.fold_in(key_list[10], 71), 0)
    return dict(node_features=node_features, norm_gain=norm_gain, norm_shift=norm_shift, query_weight=query_weight, key_value_weight=key_value_weight, out_weight=out_weight, up_weight=up_weight, down_weight=down_weight, neighbour_tiles=neighbour_tiles, neighbour_counts=neighbour_counts)


def node_norm(rows):
    average = lax.optimization_barrier(jnp.mean(rows, axis=-1, keepdims=True))
    centred = rows - average
    variance = lax.optimization_barrier(jnp.mean(centred * centred, axis=-1, keepdims=True))
    return centred * lax.rsqrt(variance + 1e-05)

def reference(node_features, norm_gain, norm_shift, query_weight, key_value_weight, out_weight, up_weight, down_weight, neighbour_tiles, neighbour_counts):
    head_size = D // HEADS
    normed = (node_norm(node_features.astype(jnp.float32)) * norm_gain).astype(jnp.bfloat16)
    query_rows = jnp.dot(normed, query_weight, preferred_element_type=jnp.float32).astype(jnp.bfloat16)
    key_value = jnp.dot(normed, key_value_weight, preferred_element_type=jnp.float32).astype(jnp.bfloat16)
    query_tiles = query_rows.reshape(TILES, TILE, HEADS, head_size)
    key_value_tiles = key_value.reshape(TILES, TILE, 2 * D)
    key_slot = (jnp.arange(NB * TILE) // TILE).astype(jnp.int32)

    def attend_tile(inputs):
        queries, tile_list, valid_count = inputs
        gathered = key_value_tiles[tile_list].reshape(NB * TILE, 2 * D)
        key_rows = gathered[:, :D].reshape(NB * TILE, HEADS, head_size).astype(jnp.float32)
        values = gathered[:, D:].reshape(NB * TILE, HEADS, head_size).astype(jnp.float32)
        scores = jnp.einsum('rhd,khd->hrk', queries.astype(jnp.float32), key_rows) / math.sqrt(head_size)
        valid = key_slot < valid_count
        scores = jnp.where(valid[None, None, :], scores, -1e+30)
        highest = lax.optimization_barrier(jnp.max(scores, axis=-1, keepdims=True))
        weights = jnp.exp(scores - highest)
        denominator = lax.optimization_barrier(jnp.sum(weights, axis=-1))
        rounded = lax.optimization_barrier(weights.astype(jnp.bfloat16))
        mixture = jnp.einsum('hrk,khd->rhd', rounded.astype(jnp.float32), values)
        mixture = mixture / denominator.T[:, :, None]
        return mixture.reshape(TILE, D).astype(jnp.bfloat16)
    attended = lax.map(attend_tile, (query_tiles, neighbour_tiles, neighbour_counts)).reshape(NODES, D)
    residual = node_features.astype(jnp.float32) + jnp.dot(attended, out_weight, preferred_element_type=jnp.float32)
    shifted = node_norm(residual) + norm_shift
    peak = lax.optimization_barrier(jnp.max(jnp.abs(shifted), axis=0))
    scaled = (4.0 * shifted / (peak + 1e-05)).astype(jnp.bfloat16)
    hidden = jax.nn.gelu(jnp.dot(scaled, up_weight, preferred_element_type=jnp.float32), approximate=True).astype(jnp.bfloat16)
    return (residual + jnp.dot(hidden, down_weight, preferred_element_type=jnp.float32)).astype(jnp.bfloat16)
```

```python
import functools
import math

import jax
import jax.numpy as jnp
from jax import lax
from jax.experimental import pallas as pl
from jax.experimental.pallas import tpu as pltpu
from jax.sharding import PartitionSpec as P

HEADS = 8
GW = 4
CAP = 4
STEPS = [(-1, -1), (-1, 0), (-1, 1), (0, -1), (0, 1), (1, -1), (1, 0), (1, 1)]
MESH = pl.DeviceIdType.MESH
VMEM = pl.BlockSpec(memory_space=pltpu.VMEM)
SMEM = pl.BlockSpec(memory_space=pltpu.SMEM)
ONES = 16


def node_norm(rows):
    average = jnp.mean(rows, axis=-1, keepdims=True)
    centred = rows - average
    variance = jnp.mean(centred * centred, axis=-1, keepdims=True)
    return centred * lax.rsqrt(variance + 1e-05)


def neighbours(group_size):
    me = lax.axis_index("blk")
    row, col = lax.div(me, GW), lax.rem(me, GW)
    grid_rows = group_size // GW
    found = []
    for dr, dc in STEPS:
        r, c = row + dr, col + dc
        ok = (r >= 0) & (r < grid_rows) & (c >= 0) & (c < GW)
        found.append((ok, jnp.where(ok, r * GW + c, me)))
    return found


def exchange_kernel(
    group_size, tiles, x, gain, wq, wkv, k_out, vt_out, qt_out, flags_out,
    marks, asked, asked_s, send, recv, fs, fr, ds, dr, local_sem,
):
    per_dev, tile_rows, width = x.shape
    slots = tiles.shape[1]
    near = neighbours(group_size)
    asked[...] = jnp.zeros_like(asked)
    barrier = pltpu.get_barrier_semaphore()
    total = jnp.int32(0)
    for ok, peer in near:
        total = total + jnp.where(ok, 1, 0)

        @pl.when(ok)
        def _():
            pl.semaphore_signal(barrier, inc=1, device_id={"blk": peer}, device_id_type=MESH)

    base = lax.axis_index("grp") * (group_size * per_dev)
    lane = lax.broadcasted_iota(jnp.int32, (group_size, 128), 1)
    line = lax.broadcasted_iota(jnp.int32, (group_size, 128), 0)
    cell = jnp.where(lane < per_dev, line * per_dev + lane + base, -1)

    def scan_row(r, found):
        for j in range(slots):
            found = jnp.where(cell == tiles[r, j], 1, found)
        return found

    found = lax.fori_loop(0, per_dev, scan_row, jnp.zeros((group_size, 128), jnp.int32))
    flags_out[...] = found
    for p in range(group_size):
        marks[p] = found[p : p + 1]
    pl.semaphore_wait(barrier, total)

    def flag_copy(s, peer):
        return pltpu.make_async_remote_copy(
            src_ref=marks.at[peer], dst_ref=asked.at[7 - s], send_sem=fs.at[s],
            recv_sem=fr.at[7 - s], device_id={"blk": peer}, device_id_type=MESH,
        )

    def flag_in(s, peer):
        return pltpu.make_async_remote_copy(
            src_ref=marks.at[peer], dst_ref=asked.at[s], send_sem=fs.at[s],
            recv_sem=fr.at[s], device_id={"blk": peer}, device_id_type=MESH,
        )

    def data_copy(s, peer):
        return pltpu.make_async_remote_copy(
            src_ref=send.at[s], dst_ref=recv.at[7 - s], send_sem=ds.at[s],
            recv_sem=dr.at[7 - s], device_id={"blk": peer}, device_id_type=MESH,
        )

    def data_in(s, peer):
        return pltpu.make_async_remote_copy(
            src_ref=send.at[s], dst_ref=recv.at[s], send_sem=ds.at[s],
            recv_sem=dr.at[s], device_id={"blk": peer}, device_id_type=MESH,
        )

    for s, (ok, peer) in enumerate(near):
        @pl.when(ok)
        def _():
            flag_copy(s, peer).start()

    for s, (ok, peer) in enumerate(near):
        @pl.when(ok)
        def _():
            flag_in(s, peer).wait_recv()

    fetch = pltpu.make_async_copy(asked, asked_s, local_sem)
    fetch.start()
    fetch.wait()
    for s, (ok, peer) in enumerate(near):
        @pl.when(ok)
        def _():
            picks = [jnp.int32(0)] * CAP
            count = jnp.int32(0)
            for t in range(per_dev):
                flag = asked_s[s, 0, t]
                for k in range(min(CAP, t + 1)):
                    picks[k] = jnp.where((flag == 1) & (count == k), t, picks[k])
                count = count + flag
            for k in range(CAP):
                send[s, k] = x[picks[k]]

    for s, (ok, peer) in enumerate(near):
        @pl.when(ok)
        def _():
            data_copy(s, peer).start()

    head_size = width // HEADS
    factor = math.log2(math.e) / math.sqrt(head_size)
    pairs = HEADS // 2

    def keys_values(normed, at):
        both = jnp.dot(normed, wkv[...], preferred_element_type=jnp.float32)
        k_out[at] = both[:, :width].astype(jnp.bfloat16)
        turned = both[:, width:].T.astype(jnp.bfloat16)
        for hp in range(pairs):
            vt_out[at, hp, : 2 * head_size] = turned[hp * 2 * head_size : (hp + 1) * 2 * head_size]
            vt_out[at, hp, 2 * head_size :] = jnp.ones((ONES, tile_rows), jnp.bfloat16)

    def normalise(rows):
        return (node_norm(rows.astype(jnp.float32)) * gain[...]).astype(jnp.bfloat16)

    def own(t, carry):
        normed = normalise(x[t])
        keys_values(normed, t)
        q = jnp.dot(normed, wq[...], preferred_element_type=jnp.float32) * factor
        qt_out[t] = q.T.astype(jnp.bfloat16)
        return carry

    lax.fori_loop(0, per_dev, own, 0)
    vt_out[per_dev + 8 * CAP] = jnp.zeros(vt_out.shape[1:], jnp.bfloat16)

    for s, (ok, peer) in enumerate(near):
        @pl.when(ok)
        def _():
            data_in(s, peer).wait_recv()

            def arrived(k, carry):
                keys_values(normalise(recv[s, k]), per_dev + s * CAP + k)
                return carry

            lax.fori_loop(0, CAP, arrived, 0)

    for s, (ok, peer) in enumerate(near):
        @pl.when(ok)
        def _():
            flag_copy(s, peer).wait_send()
            data_copy(s, peer).wait_send()


def attend_kernel(
    group_size, tiles, counts, flags, keys, vt, qt, x, wo, shift, res_out, peak_out,
    pos, qbd, acc, top,
):
    per_dev, tile_rows, width = x.shape
    head_size = width // HEADS
    pairs = HEADS // 2
    two = 2 * head_size
    me = lax.axis_index("blk")
    base = lax.axis_index("grp") * (group_size * per_dev)
    null = per_dev + 8 * CAP
    for t in range(per_dev):
        pos[me * per_dev + t] = t
    for s, (ok, peer) in enumerate(neighbours(group_size)):
        @pl.when(ok)
        def _():
            place = jnp.int32(per_dev + s * CAP)
            for t in range(per_dev):
                pos[peer * per_dev + t] = place
                place = place + flags[peer, t]

    peak_out[...] = jnp.zeros_like(peak_out)
    feature = lax.broadcasted_iota(jnp.int32, (width, tile_rows), 0) // head_size

    def one_tile(t, carry):
        q = qt[t]
        for h in range(HEADS):
            qbd[:, h * tile_rows : (h + 1) * tile_rows] = jnp.where(
                feature == h, q, jnp.zeros_like(q)
            )
        acc[...] = jnp.zeros_like(acc)
        top[...] = jnp.full_like(top, -1e30)
        count = counts[t]

        def visit(c, carry):
            first = pos[tiles[t, 2 * c] - base]
            second = pos[tiles[t, 2 * c + 1] - base]
            second_v = jnp.where(2 * c + 1 < count, second, null)
            k2 = jnp.concatenate([keys[first], keys[second]], axis=0)
            for hp in range(pairs):
                cols = slice(hp * 2 * tile_rows, (hp + 1) * 2 * tile_rows)
                scores = jnp.dot(k2, qbd[:, cols], preferred_element_type=jnp.float32)
                old = top[hp]
                new = jnp.maximum(old, jnp.max(scores, axis=0, keepdims=True))
                weights = jnp.exp2(scores - new).astype(jnp.bfloat16)
                v2 = jnp.concatenate([vt[first, hp], vt[second_v, hp]], axis=1)
                mixed = jnp.dot(v2, weights, preferred_element_type=jnp.float32)
                acc[hp] = acc[hp] * jnp.exp2(old - new) + mixed
                top[hp] = new
            return carry

        lax.fori_loop(0, (count + 1) // 2, visit, 0)
        parts = []
        for hp in range(pairs):
            for side in range(2):
                lanes = slice(side * tile_rows, (side + 1) * tile_rows)
                rows = slice(side * head_size, (side + 1) * head_size)
                parts.append(acc[hp, rows, lanes] / acc[hp, two : two + 1, lanes])
        attended = jnp.concatenate(parts, axis=0).T.astype(jnp.bfloat16)
        residual = x[t].astype(jnp.float32) + jnp.dot(
            attended, wo[...], preferred_element_type=jnp.float32
        )
        res_out[t] = residual
        shifted = node_norm(residual) + shift[...]
        peak_out[...] = jnp.maximum(
            peak_out[...], jnp.max(jnp.abs(shifted), axis=0, keepdims=True)
        )
        return carry

    lax.fori_loop(0, per_dev, one_tile, 0)


def peak_kernel(groups, group_size, local, out, got, send_sem, recv_sem):
    grp, blk = lax.axis_index("grp"), lax.axis_index("blk")
    others = [
        (g, b) for g in range(groups) for b in range(group_size) if (g, b) != (0, 0)
    ]

    def target(g, b):
        return {"grp": lax.rem(grp + g, groups), "blk": lax.rem(blk + b, group_size)}

    barrier = pltpu.get_barrier_semaphore()
    for g, b in others:
        pl.semaphore_signal(barrier, inc=1, device_id=target(g, b), device_id_type=MESH)
    pl.semaphore_wait(barrier, len(others))
    copies = []
    for i, (g, b) in enumerate(others):
        copy = pltpu.make_async_remote_copy(
            src_ref=local, dst_ref=got.at[i], send_sem=send_sem.at[i],
            recv_sem=recv_sem.at[i], device_id=target(g, b), device_id_type=MESH,
        )
        copy.start()
        copies.append(copy)
    best = local[...]
    for i, copy in enumerate(copies):
        copy.wait_recv()
        best = jnp.maximum(best, got[i])
    out[...] = best
    for copy in copies:
        copy.wait_send()


def mlp_kernel(res, peak, shift, up, down, out):
    residual = res[0]
    shifted = node_norm(residual) + shift[...]
    scaled = (4.0 * shifted / (peak[...] + 1e-05)).astype(jnp.bfloat16)
    h = jnp.dot(scaled, up[...], preferred_element_type=jnp.float32)
    h = jax.nn.gelu(h, approximate=True).astype(jnp.bfloat16)
    out[...] = (residual + jnp.dot(h, down[...], preferred_element_type=jnp.float32)).astype(
        jnp.bfloat16
    )


def shards(
    groups, group_size, node_features, norm_gain, norm_shift, query_weight, key_value_weight,
    out_weight, up_weight, down_weight, neighbour_tiles, neighbour_counts,
):
    per_dev = neighbour_tiles.shape[0]
    rows, width = node_features.shape
    tile_rows = rows // per_dev
    pairs = HEADS // 2
    aug = 2 * (width // HEADS) + ONES
    table = per_dev + 8 * CAP
    x = node_features.reshape(per_dev, tile_rows, width)
    gain = norm_gain.reshape(1, width)
    shift = norm_shift.reshape(1, width)
    bf16, f32, i32 = jnp.bfloat16, jnp.float32, jnp.int32
    limit = 24 * 1024 * 1024
    keys, vt, qt, flags = pl.pallas_call(
        functools.partial(exchange_kernel, group_size),
        out_shape=(
            jax.ShapeDtypeStruct((table, tile_rows, width), bf16),
            jax.ShapeDtypeStruct((table + 1, pairs, aug, tile_rows), bf16),
            jax.ShapeDtypeStruct((per_dev, width, tile_rows), bf16),
            jax.ShapeDtypeStruct((group_size, 128), i32),
        ),
        in_specs=[SMEM] + [VMEM] * 4,
        out_specs=(VMEM,) * 4,
        scratch_shapes=[
            pltpu.VMEM((group_size, 1, 128), i32),
            pltpu.VMEM((8, 1, 128), i32),
            pltpu.SMEM((8, 1, 128), i32),
            pltpu.VMEM((8, CAP, tile_rows, width), bf16),
            pltpu.VMEM((8, CAP, tile_rows, width), bf16),
            pltpu.SemaphoreType.DMA((8,)),
            pltpu.SemaphoreType.DMA((8,)),
            pltpu.SemaphoreType.DMA((8,)),
            pltpu.SemaphoreType.DMA((8,)),
            pltpu.SemaphoreType.DMA,
        ],
        compiler_params=pltpu.CompilerParams(
            collective_id=0, has_side_effects=True, vmem_limit_bytes=limit
        ),
        name="exchange",
    )(neighbour_tiles, x, gain, query_weight, key_value_weight)
    residual, local_peak = pl.pallas_call(
        functools.partial(attend_kernel, group_size),
        out_shape=(
            jax.ShapeDtypeStruct((per_dev, tile_rows, width), f32),
            jax.ShapeDtypeStruct((1, width), f32),
        ),
        in_specs=[SMEM] * 3 + [VMEM] * 6,
        out_specs=(VMEM,) * 2,
        scratch_shapes=[
            pltpu.SMEM((group_size * per_dev,), i32),
            pltpu.VMEM((width, HEADS * tile_rows), bf16),
            pltpu.VMEM((pairs, aug, 2 * tile_rows), f32),
            pltpu.VMEM((pairs, 1, 2 * tile_rows), f32),
        ],
        compiler_params=pltpu.CompilerParams(vmem_limit_bytes=limit),
        name="attend",
    )(
        neighbour_tiles, neighbour_counts, flags, keys, vt, qt, x, out_weight, shift
    )
    count = groups * group_size - 1
    peak = pl.pallas_call(
        functools.partial(peak_kernel, groups, group_size),
        out_shape=jax.ShapeDtypeStruct((1, width), f32),
        in_specs=[VMEM],
        out_specs=VMEM,
        scratch_shapes=[
            pltpu.VMEM((count, 1, width), f32),
            pltpu.SemaphoreType.DMA((count,)),
            pltpu.SemaphoreType.DMA((count,)),
        ],
        compiler_params=pltpu.CompilerParams(collective_id=1, has_side_effects=True),
        name="peak",
    )(local_peak)
    whole = lambda *shape: pl.BlockSpec(shape, lambda i: (0,) * len(shape))
    return pl.pallas_call(
        mlp_kernel,
        grid=(per_dev,),
        out_shape=jax.ShapeDtypeStruct((rows, width), bf16),
        in_specs=[
            pl.BlockSpec((1, tile_rows, width), lambda i: (i, 0, 0)),
            whole(1, width),
            whole(1, width),
            whole(*up_weight.shape),
            whole(*down_weight.shape),
        ],
        out_specs=pl.BlockSpec((tile_rows, width), lambda i: (i, 0)),
        compiler_params=pltpu.CompilerParams(vmem_limit_bytes=limit),
        name="mlp",
    )(residual, peak, shift, up_weight, down_weight)


def solution(mesh):
    split = P(("grp", "blk"), None)
    body = functools.partial(shards, mesh.shape["grp"], mesh.shape["blk"])
    return jax.shard_map(
        body,
        mesh=mesh,
        in_specs=(split, P(), P(), P(), P(), P(), P(), P(), split, P(("grp", "blk"))),
        out_specs=split,
        check_vma=False,
    )
```

```python
import functools
import math

import jax
import jax.numpy as jnp
from jax import lax
from jax.experimental import pallas as pl
from jax.experimental.pallas import tpu as pltpu
from jax.sharding import PartitionSpec as P

HEADS = 8
GW = 4
CAP = 4
STEPS = [(-1, -1), (-1, 0), (-1, 1), (0, -1), (0, 1), (1, -1), (1, 0), (1, 1)]
MESH = pl.DeviceIdType.MESH
VMEM = pl.BlockSpec(memory_space=pltpu.VMEM)
SMEM = pl.BlockSpec(memory_space=pltpu.SMEM)
ONES = 16


def node_norm(rows):
    average = jnp.mean(rows, axis=-1, keepdims=True)
    centred = rows - average
    variance = jnp.mean(centred * centred, axis=-1, keepdims=True)
    return centred * lax.rsqrt(variance + 1e-05)


def neighbours(group_size):
    me = lax.axis_index("blk")
    row, col = lax.div(me, GW), lax.rem(me, GW)
    grid_rows = group_size // GW
    found = []
    for dr, dc in STEPS:
        r, c = row + dr, col + dc
        ok = (r >= 0) & (r < grid_rows) & (c >= 0) & (c < GW)
        found.append((ok, jnp.where(ok, r * GW + c, me)))
    return found


def exchange_kernel(
    group_size, tiles, x, gain, wq, wkv, k_out, vt_out, qt_out, flags_out,
    marks, asked, asked_s, send, recv, fs, fr, ds, dr, local_sem,
):
    per_dev, tile_rows, width = x.shape
    slots = tiles.shape[1]
    near = neighbours(group_size)
    asked[...] = jnp.zeros_like(asked)
    barrier = pltpu.get_barrier_semaphore()
    total = jnp.int32(0)
    for ok, peer in near:
        total = total + jnp.where(ok, 1, 0)

        @pl.when(ok)
        def _():
            pl.semaphore_signal(barrier, inc=1, device_id={"blk": peer}, device_id_type=MESH)

    base = lax.axis_index("grp") * (group_size * per_dev)
    lane = lax.broadcasted_iota(jnp.int32, (group_size, 128), 1)
    line = lax.broadcasted_iota(jnp.int32, (group_size, 128), 0)
    cell = jnp.where(lane < per_dev, line * per_dev + lane + base, -1)

    def scan_row(r, found):
        for j in range(slots):
            found = jnp.where(cell == tiles[r, j], 1, found)
        return found

    found = lax.fori_loop(0, per_dev, scan_row, jnp.zeros((group_size, 128), jnp.int32))
    flags_out[...] = found
    for p in range(group_size):
        marks[p] = found[p : p + 1]
    pl.semaphore_wait(barrier, total)

    def flag_copy(s, peer):
        return pltpu.make_async_remote_copy(
            src_ref=marks.at[peer], dst_ref=asked.at[7 - s], send_sem=fs.at[s],
            recv_sem=fr.at[7 - s], device_id={"blk": peer}, device_id_type=MESH,
        )

    def flag_in(s, peer):
        return pltpu.make_async_remote_copy(
            src_ref=marks.at[peer], dst_ref=asked.at[s], send_sem=fs.at[s],
            recv_sem=fr.at[s], device_id={"blk": peer}, device_id_type=MESH,
        )

    def data_copy(s, peer):
        return pltpu.make_async_remote_copy(
            src_ref=send.at[s], dst_ref=recv.at[7 - s], send_sem=ds.at[s],
            recv_sem=dr.at[7 - s], device_id={"blk": peer}, device_id_type=MESH,
        )

    def data_in(s, peer):
        return pltpu.make_async_remote_copy(
            src_ref=send.at[s], dst_ref=recv.at[s], send_sem=ds.at[s],
            recv_sem=dr.at[s], device_id={"blk": peer}, device_id_type=MESH,
        )

    for s, (ok, peer) in enumerate(near):
        @pl.when(ok)
        def _():
            flag_copy(s, peer).start()

    for s, (ok, peer) in enumerate(near):
        @pl.when(ok)
        def _():
            flag_in(s, peer).wait_recv()

    fetch = pltpu.make_async_copy(asked, asked_s, local_sem)
    fetch.start()
    fetch.wait()
    for s, (ok, peer) in enumerate(near):
        @pl.when(ok)
        def _():
            picks = [jnp.int32(0)] * CAP
            count = jnp.int32(0)
            for t in range(per_dev):
                flag = asked_s[s, 0, t]
                for k in range(min(CAP, t + 1)):
                    picks[k] = jnp.where((flag == 1) & (count == k), t, picks[k])
                count = count + flag
            for k in range(CAP):
                send[s, k] = x[picks[k]]

    for s, (ok, peer) in enumerate(near):
        @pl.when(ok)
        def _():
            data_copy(s, peer).start()

    head_size = width // HEADS
    factor = math.log2(math.e) / math.sqrt(head_size)
    pairs = HEADS // 2

    def keys_values(normed, at):
        both = jnp.dot(normed, wkv[...], preferred_element_type=jnp.float32)
        k_out[at] = both[:, :width].astype(jnp.bfloat16)
        turned = both[:, width:].T.astype(jnp.bfloat16)
        for hp in range(pairs):
            vt_out[at, hp, : 2 * head_size] = turned[hp * 2 * head_size : (hp + 1) * 2 * head_size]
            vt_out[at, hp, 2 * head_size :] = jnp.ones((ONES, tile_rows), jnp.bfloat16)

    def normalise(rows):
        return (node_norm(rows.astype(jnp.float32)) * gain[...]).astype(jnp.bfloat16)

    def own(t, carry):
        normed = normalise(x[t])
        keys_values(normed, t)
        q = jnp.dot(normed, wq[...], preferred_element_type=jnp.float32) * factor
        qt_out[t] = q.T.astype(jnp.bfloat16)
        return carry

    lax.fori_loop(0, per_dev, own, 0)
    vt_out[per_dev + 8 * CAP] = jnp.zeros(vt_out.shape[1:], jnp.bfloat16)

    for s, (ok, peer) in enumerate(near):
        @pl.when(ok)
        def _():
            data_in(s, peer).wait_recv()

            def arrived(k, carry):
                keys_values(normalise(recv[s, k]), per_dev + s * CAP + k)
                return carry

            lax.fori_loop(0, CAP, arrived, 0)

    for s, (ok, peer) in enumerate(near):
        @pl.when(ok)
        def _():
            flag_copy(s, peer).wait_send()
            data_copy(s, peer).wait_send()


def attend_kernel(
    group_size, tiles, counts, flags, keys, vt, qt, x, wo, shift, res_out, peak_out,
    pos, qbd, acc, top, fresh, held_a, held_b,
):
    per_dev, tile_rows, width = x.shape
    head_size = width // HEADS
    pairs = HEADS // 2
    two = 2 * head_size
    me = lax.axis_index("blk")
    base = lax.axis_index("grp") * (group_size * per_dev)
    null = per_dev + 8 * CAP
    for t in range(per_dev):
        pos[me * per_dev + t] = t
    for s, (ok, peer) in enumerate(neighbours(group_size)):
        @pl.when(ok)
        def _():
            place = jnp.int32(per_dev + s * CAP)
            for t in range(per_dev):
                pos[peer * per_dev + t] = place
                place = place + flags[peer, t]

    peak_out[...] = jnp.zeros_like(peak_out)
    feature = lax.broadcasted_iota(jnp.int32, (width, tile_rows), 0) // head_size

    def one_tile(t, carry):
        q = qt[t]
        for h in range(HEADS):
            qbd[:, h * tile_rows : (h + 1) * tile_rows] = jnp.where(
                feature == h, q, jnp.zeros_like(q)
            )
        acc[...] = jnp.zeros_like(acc)
        top[...] = jnp.full_like(top, -1e30)
        count = counts[t]
        chunks = (count + 1) // 2

        def place(slot):
            return pos[tiles[t, slot] - base]

        def score(c, quad, held):
            k2 = jnp.concatenate([keys[place(2 * c)], keys[place(2 * c + 1)]], axis=0)
            cols = slice(quad * 4 * tile_rows, (quad + 1) * 4 * tile_rows)
            scores = jnp.dot(k2, qbd[:, cols], preferred_element_type=jnp.float32)
            held[...] = scores
            fresh[quad] = jnp.max(scores, axis=0, keepdims=True)

        def mix(c, quad, held):
            first = place(2 * c)
            second = jnp.where(2 * c + 1 < count, place(2 * c + 1), null)
            old = top[quad]
            new = jnp.maximum(old, fresh[quad])
            top[quad] = new
            decay = jnp.exp2(old - new)
            for side in range(2):
                hp = 2 * quad + side
                cols = slice(side * 2 * tile_rows, (side + 1) * 2 * tile_rows)
                weights = jnp.exp2(held[:, cols] - new[:, cols]).astype(jnp.bfloat16)
                v2 = jnp.concatenate([vt[first, hp], vt[second, hp]], axis=1)
                mixed = jnp.dot(v2, weights, preferred_element_type=jnp.float32)
                acc[hp] = acc[hp] * decay[:, cols] + mixed

        def visit(c, carry):
            score(c, 1, held_b)
            mix(c, 0, held_a)
            score(jnp.minimum(c + 1, chunks - 1), 0, held_a)
            mix(c, 1, held_b)
            return carry

        score(0, 0, held_a)
        lax.fori_loop(0, chunks, visit, 0)
        parts = []
        for hp in range(pairs):
            for side in range(2):
                lanes = slice(side * tile_rows, (side + 1) * tile_rows)
                rows = slice(side * head_size, (side + 1) * head_size)
                parts.append(acc[hp, rows, lanes] / acc[hp, two : two + 1, lanes])
        attended = jnp.concatenate(parts, axis=0).T.astype(jnp.bfloat16)
        residual = x[t].astype(jnp.float32) + jnp.dot(
            attended, wo[...], preferred_element_type=jnp.float32
        )
        res_out[t] = residual
        shifted = node_norm(residual) + shift[...]
        peak_out[...] = jnp.maximum(
            peak_out[...], jnp.max(jnp.abs(shifted), axis=0, keepdims=True)
        )
        return carry

    lax.fori_loop(0, per_dev, one_tile, 0)


def peak_kernel(groups, group_size, local, out, mine, got, own_sem, gs, gr, bs, br):
    grp, blk = lax.axis_index("grp"), lax.axis_index("blk")

    def along(name, at, count, step):
        return {name: lax.rem(at + step, count)}

    barrier = pltpu.get_barrier_semaphore()
    for g in range(1, groups):
        pl.semaphore_signal(
            barrier, inc=1, device_id=along("grp", grp, groups, g), device_id_type=MESH
        )
    for b in range(1, group_size):
        pl.semaphore_signal(
            barrier, inc=1, device_id=along("blk", blk, group_size, b), device_id_type=MESH
        )
    own = pltpu.make_async_copy(local, mine.at[0], own_sem)
    own.start()
    pl.semaphore_wait(barrier, groups + group_size - 2)
    copies = []
    for g in range(1, groups):
        copy = pltpu.make_async_remote_copy(
            src_ref=local, dst_ref=mine.at[g], send_sem=gs.at[g], recv_sem=gr.at[g],
            device_id=along("grp", grp, groups, g), device_id_type=MESH,
        )
        copy.start()
        copies.append(copy)
    own.wait()
    for copy in copies:
        copy.wait_recv()
    far = []
    for b in range(1, group_size):
        copy = pltpu.make_async_remote_copy(
            src_ref=mine, dst_ref=got.at[b - 1], send_sem=bs.at[b], recv_sem=br.at[b],
            device_id=along("blk", blk, group_size, b), device_id_type=MESH,
        )
        copy.start()
        far.append(copy)
    best = jnp.max(mine[...], axis=0)
    for b, copy in enumerate(far):
        copy.wait_recv()
        best = jnp.maximum(best, jnp.max(got[b], axis=0))
    out[...] = best
    for copy in copies + far:
        copy.wait_send()


def mlp_kernel(res, peak, shift, up, down, out):
    residual = res[0]
    shifted = node_norm(residual) + shift[...]
    scaled = (4.0 * shifted / (peak[...] + 1e-05)).astype(jnp.bfloat16)
    h = jnp.dot(scaled, up[...], preferred_element_type=jnp.float32)
    h = jax.nn.gelu(h, approximate=True).astype(jnp.bfloat16)
    out[...] = (residual + jnp.dot(h, down[...], preferred_element_type=jnp.float32)).astype(
        jnp.bfloat16
    )


def shards(
    groups, group_size, node_features, norm_gain, norm_shift, query_weight, key_value_weight,
    out_weight, up_weight, down_weight, neighbour_tiles, neighbour_counts,
):
    per_dev = neighbour_tiles.shape[0]
    rows, width = node_features.shape
    tile_rows = rows // per_dev
    pairs = HEADS // 2
    aug = 2 * (width // HEADS) + ONES
    table = per_dev + 8 * CAP
    x = node_features.reshape(per_dev, tile_rows, width)
    gain = norm_gain.reshape(1, width)
    shift = norm_shift.reshape(1, width)
    bf16, f32, i32 = jnp.bfloat16, jnp.float32, jnp.int32
    limit = 24 * 1024 * 1024
    keys, vt, qt, flags = pl.pallas_call(
        functools.partial(exchange_kernel, group_size),
        out_shape=(
            jax.ShapeDtypeStruct((table, tile_rows, width), bf16),
            jax.ShapeDtypeStruct((table + 1, pairs, aug, tile_rows), bf16),
            jax.ShapeDtypeStruct((per_dev, width, tile_rows), bf16),
            jax.ShapeDtypeStruct((group_size, 128), i32),
        ),
        in_specs=[SMEM] + [VMEM] * 4,
        out_specs=(VMEM,) * 4,
        scratch_shapes=[
            pltpu.VMEM((group_size, 1, 128), i32),
            pltpu.VMEM((8, 1, 128), i32),
            pltpu.SMEM((8, 1, 128), i32),
            pltpu.VMEM((8, CAP, tile_rows, width), bf16),
            pltpu.VMEM((8, CAP, tile_rows, width), bf16),
            pltpu.SemaphoreType.DMA((8,)),
            pltpu.SemaphoreType.DMA((8,)),
            pltpu.SemaphoreType.DMA((8,)),
            pltpu.SemaphoreType.DMA((8,)),
            pltpu.SemaphoreType.DMA,
        ],
        compiler_params=pltpu.CompilerParams(
            collective_id=0, has_side_effects=True, vmem_limit_bytes=limit
        ),
        name="exchange",
    )(neighbour_tiles, x, gain, query_weight, key_value_weight)
    residual, local_peak = pl.pallas_call(
        functools.partial(attend_kernel, group_size),
        out_shape=(
            jax.ShapeDtypeStruct((per_dev, tile_rows, width), f32),
            jax.ShapeDtypeStruct((1, width), f32),
        ),
        in_specs=[SMEM] * 3 + [VMEM] * 6,
        out_specs=(VMEM,) * 2,
        scratch_shapes=[
            pltpu.SMEM((group_size * per_dev,), i32),
            pltpu.VMEM((width, HEADS * tile_rows), bf16),
            pltpu.VMEM((pairs, aug, 2 * tile_rows), f32),
            pltpu.VMEM((2, 1, 4 * tile_rows), f32),
            pltpu.VMEM((2, 1, 4 * tile_rows), f32),
            pltpu.VMEM((2 * tile_rows, 4 * tile_rows), f32),
            pltpu.VMEM((2 * tile_rows, 4 * tile_rows), f32),
        ],
        compiler_params=pltpu.CompilerParams(vmem_limit_bytes=limit),
        name="attend",
    )(
        neighbour_tiles, neighbour_counts, flags, keys, vt, qt, x, out_weight, shift
    )
    peak = pl.pallas_call(
        functools.partial(peak_kernel, groups, group_size),
        out_shape=jax.ShapeDtypeStruct((1, width), f32),
        in_specs=[VMEM],
        out_specs=VMEM,
        scratch_shapes=[
            pltpu.VMEM((groups, 1, width), f32),
            pltpu.VMEM((group_size - 1, groups, 1, width), f32),
            pltpu.SemaphoreType.DMA,
            pltpu.SemaphoreType.DMA((groups,)),
            pltpu.SemaphoreType.DMA((groups,)),
            pltpu.SemaphoreType.DMA((group_size,)),
            pltpu.SemaphoreType.DMA((group_size,)),
        ],
        compiler_params=pltpu.CompilerParams(collective_id=1, has_side_effects=True),
        name="peak",
    )(local_peak)
    whole = lambda *shape: pl.BlockSpec(shape, lambda i: (0,) * len(shape))
    return pl.pallas_call(
        mlp_kernel,
        grid=(per_dev,),
        out_shape=jax.ShapeDtypeStruct((rows, width), bf16),
        in_specs=[
            pl.BlockSpec((1, tile_rows, width), lambda i: (i, 0, 0)),
            whole(1, width),
            whole(1, width),
            whole(*up_weight.shape),
            whole(*down_weight.shape),
        ],
        out_specs=pl.BlockSpec((tile_rows, width), lambda i: (i, 0)),
        compiler_params=pltpu.CompilerParams(vmem_limit_bytes=limit),
        name="mlp",
    )(residual, peak, shift, up_weight, down_weight)


def solution(mesh):
    split = P(("grp", "blk"), None)
    body = functools.partial(shards, mesh.shape["grp"], mesh.shape["blk"])
    return jax.shard_map(
        body,
        mesh=mesh,
        in_specs=(split, P(), P(), P(), P(), P(), P(), P(), split, P(("grp", "blk"))),
        out_specs=split,
        check_vma=False,
    )
```

```python
import functools
import math

import jax
import jax.numpy as jnp
from jax import lax
from jax.experimental import pallas as pl
from jax.experimental.pallas import tpu as pltpu
from jax.sharding import PartitionSpec as P

HEADS = 8
GW = 4
CAP = 4
STEPS = [(-1, -1), (-1, 0), (-1, 1), (0, -1), (0, 1), (1, -1), (1, 0), (1, 1)]
MESH = pl.DeviceIdType.MESH
VMEM = pl.BlockSpec(memory_space=pltpu.VMEM)
SMEM = pl.BlockSpec(memory_space=pltpu.SMEM)
ONES = 16


def node_norm(rows):
    average = jnp.mean(rows, axis=-1, keepdims=True)
    centred = rows - average
    variance = jnp.mean(centred * centred, axis=-1, keepdims=True)
    return centred * lax.rsqrt(variance + 1e-05)


def neighbours(group_size):
    me = lax.axis_index("blk")
    row, col = lax.div(me, GW), lax.rem(me, GW)
    grid_rows = group_size // GW
    found = []
    for dr, dc in STEPS:
        r, c = row + dr, col + dc
        ok = (r >= 0) & (r < grid_rows) & (c >= 0) & (c < GW)
        found.append((ok, jnp.where(ok, r * GW + c, me)))
    return found


def exchange_kernel(
    group_size, tiles, x, gain, wq, wkv, k_out, vt_out, qt_out, flags_out,
    marks, asked, asked_s, send, recv, fs, fr, ds, dr, local_sem,
):
    per_dev, tile_rows, width = x.shape
    slots = tiles.shape[1]
    near = neighbours(group_size)
    asked[...] = jnp.zeros_like(asked)
    barrier = pltpu.get_barrier_semaphore()
    total = jnp.int32(0)
    for ok, peer in near:
        total = total + jnp.where(ok, 1, 0)

        @pl.when(ok)
        def _():
            pl.semaphore_signal(barrier, inc=1, device_id={"blk": peer}, device_id_type=MESH)

    base = lax.axis_index("grp") * (group_size * per_dev)
    lane = lax.broadcasted_iota(jnp.int32, (group_size, 128), 1)
    line = lax.broadcasted_iota(jnp.int32, (group_size, 128), 0)
    cell = jnp.where(lane < per_dev, line * per_dev + lane + base, -1)

    def scan_row(r, found):
        for j in range(slots):
            found = jnp.where(cell == tiles[r, j], 1, found)
        return found

    found = lax.fori_loop(0, per_dev, scan_row, jnp.zeros((group_size, 128), jnp.int32))
    flags_out[...] = found
    for p in range(group_size):
        marks[p] = found[p : p + 1]
    pl.semaphore_wait(barrier, total)

    def flag_copy(s, peer):
        return pltpu.make_async_remote_copy(
            src_ref=marks.at[peer], dst_ref=asked.at[7 - s], send_sem=fs.at[s],
            recv_sem=fr.at[7 - s], device_id={"blk": peer}, device_id_type=MESH,
        )

    def flag_in(s, peer):
        return pltpu.make_async_remote_copy(
            src_ref=marks.at[peer], dst_ref=asked.at[s], send_sem=fs.at[s],
            recv_sem=fr.at[s], device_id={"blk": peer}, device_id_type=MESH,
        )

    def data_copy(s, peer):
        return pltpu.make_async_remote_copy(
            src_ref=send.at[s], dst_ref=recv.at[7 - s], send_sem=ds.at[s],
            recv_sem=dr.at[7 - s], device_id={"blk": peer}, device_id_type=MESH,
        )

    def data_in(s, peer):
        return pltpu.make_async_remote_copy(
            src_ref=send.at[s], dst_ref=recv.at[s], send_sem=ds.at[s],
            recv_sem=dr.at[s], device_id={"blk": peer}, device_id_type=MESH,
        )

    for s, (ok, peer) in enumerate(near):
        @pl.when(ok)
        def _():
            flag_copy(s, peer).start()

    for s, (ok, peer) in enumerate(near):
        @pl.when(ok)
        def _():
            flag_in(s, peer).wait_recv()

    fetch = pltpu.make_async_copy(asked, asked_s, local_sem)
    fetch.start()
    fetch.wait()
    for s, (ok, peer) in enumerate(near):
        @pl.when(ok)
        def _():
            picks = [jnp.int32(0)] * CAP
            count = jnp.int32(0)
            for t in range(per_dev):
                flag = asked_s[s, 0, t]
                for k in range(min(CAP, t + 1)):
                    picks[k] = jnp.where((flag == 1) & (count == k), t, picks[k])
                count = count + flag
            for k in range(CAP):
                send[s, k] = x[picks[k]]

    for s, (ok, peer) in enumerate(near):
        @pl.when(ok)
        def _():
            data_copy(s, peer).start()

    head_size = width // HEADS
    factor = math.log2(math.e) / math.sqrt(head_size)
    pairs = HEADS // 2

    def keys_values(normed, at):
        both = jnp.dot(normed, wkv[...], preferred_element_type=jnp.float32)
        k_out[at] = both[:, :width].astype(jnp.bfloat16)
        turned = both[:, width:].T.astype(jnp.bfloat16)
        for hp in range(pairs):
            vt_out[at, hp, : 2 * head_size] = turned[hp * 2 * head_size : (hp + 1) * 2 * head_size]
            vt_out[at, hp, 2 * head_size :] = jnp.ones((ONES, tile_rows), jnp.bfloat16)

    def normalise(rows):
        return (node_norm(rows.astype(jnp.float32)) * gain[...]).astype(jnp.bfloat16)

    def own(t, carry):
        normed = normalise(x[t])
        keys_values(normed, t)
        q = jnp.dot(normed, wq[...], preferred_element_type=jnp.float32) * factor
        qt_out[t] = q.T.astype(jnp.bfloat16)
        return carry

    lax.fori_loop(0, per_dev, own, 0, unroll=2)
    vt_out[per_dev + 8 * CAP] = jnp.zeros(vt_out.shape[1:], jnp.bfloat16)

    for s in (3, 4, 1, 6, 0, 2, 5, 7):
        ok, peer = near[s]

        @pl.when(ok)
        def _():
            data_in(s, peer).wait_recv()

            def arrived(k, carry):
                keys_values(normalise(recv[s, k]), per_dev + s * CAP + k)
                return carry

            lax.fori_loop(0, CAP, arrived, 0, unroll=2)

    for s, (ok, peer) in enumerate(near):
        @pl.when(ok)
        def _():
            flag_copy(s, peer).wait_send()
            data_copy(s, peer).wait_send()


def attend_kernel(
    group_size, tiles, counts, flags, keys, vt, qt, x, wo, shift, res_out, peak_out,
    pos, qbd, acc, top, fresh, held_a, held_b,
):
    per_dev, tile_rows, width = x.shape
    head_size = width // HEADS
    pairs = HEADS // 2
    two = 2 * head_size
    me = lax.axis_index("blk")
    base = lax.axis_index("grp") * (group_size * per_dev)
    null = per_dev + 8 * CAP
    for t in range(per_dev):
        pos[me * per_dev + t] = t
    for s, (ok, peer) in enumerate(neighbours(group_size)):
        @pl.when(ok)
        def _():
            place = jnp.int32(per_dev + s * CAP)
            for t in range(per_dev):
                pos[peer * per_dev + t] = place
                place = place + flags[peer, t]

    peak_out[...] = jnp.zeros_like(peak_out)
    feature = lax.broadcasted_iota(jnp.int32, (width, tile_rows), 0) // head_size

    def one_tile(t, carry):
        q = qt[t]
        for h in range(HEADS):
            qbd[:, h * tile_rows : (h + 1) * tile_rows] = jnp.where(
                feature == h, q, jnp.zeros_like(q)
            )
        acc[...] = jnp.zeros_like(acc)
        top[...] = jnp.full_like(top, -1e30)
        count = counts[t]
        chunks = (count + 1) // 2

        def place(slot):
            return pos[tiles[t, slot] - base]

        def score(c, quad, held):
            k2 = jnp.concatenate([keys[place(2 * c)], keys[place(2 * c + 1)]], axis=0)
            cols = slice(quad * 4 * tile_rows, (quad + 1) * 4 * tile_rows)
            scores = jnp.dot(k2, qbd[:, cols], preferred_element_type=jnp.float32)
            held[...] = scores
            fresh[quad] = jnp.max(scores, axis=0, keepdims=True)

        def mix(c, quad, held):
            first = place(2 * c)
            second = jnp.where(2 * c + 1 < count, place(2 * c + 1), null)
            old = top[quad]
            new = jnp.maximum(old, fresh[quad])
            top[quad] = new
            decay = jnp.exp2(old - new)
            for side in range(2):
                hp = 2 * quad + side
                cols = slice(side * 2 * tile_rows, (side + 1) * 2 * tile_rows)
                weights = jnp.exp2(held[:, cols] - new[:, cols]).astype(jnp.bfloat16)
                v2 = jnp.concatenate([vt[first, hp], vt[second, hp]], axis=1)
                mixed = jnp.dot(v2, weights, preferred_element_type=jnp.float32)
                acc[hp] = acc[hp] * decay[:, cols] + mixed

        def visit(c, carry):
            score(c, 1, held_b)
            mix(c, 0, held_a)
            score(jnp.minimum(c + 1, chunks - 1), 0, held_a)
            mix(c, 1, held_b)
            return carry

        score(0, 0, held_a)
        lax.fori_loop(0, chunks, visit, 0)
        parts = []
        for hp in range(pairs):
            for side in range(2):
                lanes = slice(side * tile_rows, (side + 1) * tile_rows)
                rows = slice(side * head_size, (side + 1) * head_size)
                parts.append(acc[hp, rows, lanes] / acc[hp, two : two + 1, lanes])
        attended = jnp.concatenate(parts, axis=0).T.astype(jnp.bfloat16)
        residual = x[t].astype(jnp.float32) + jnp.dot(
            attended, wo[...], preferred_element_type=jnp.float32
        )
        res_out[t] = residual
        shifted = node_norm(residual) + shift[...]
        peak_out[...] = jnp.maximum(
            peak_out[...], jnp.max(jnp.abs(shifted), axis=0, keepdims=True)
        )
        return carry

    lax.fori_loop(0, per_dev, one_tile, 0)


def peak_kernel(groups, group_size, local, out, mine, got, own_sem, gs, gr, bs, br):
    grp, blk = lax.axis_index("grp"), lax.axis_index("blk")

    def along(name, at, count, step):
        return {name: lax.rem(at + step, count)}

    barrier = pltpu.get_barrier_semaphore()
    for g in range(1, groups):
        pl.semaphore_signal(
            barrier, inc=1, device_id=along("grp", grp, groups, g), device_id_type=MESH
        )
    for b in range(1, group_size):
        pl.semaphore_signal(
            barrier, inc=1, device_id=along("blk", blk, group_size, b), device_id_type=MESH
        )
    own = pltpu.make_async_copy(local, mine.at[0], own_sem)
    own.start()
    pl.semaphore_wait(barrier, groups + group_size - 2)
    copies = []
    for g in range(1, groups):
        copy = pltpu.make_async_remote_copy(
            src_ref=local, dst_ref=mine.at[g], send_sem=gs.at[g], recv_sem=gr.at[g],
            device_id=along("grp", grp, groups, g), device_id_type=MESH,
        )
        copy.start()
        copies.append(copy)
    own.wait()
    for copy in copies:
        copy.wait_recv()
    far = []
    for b in range(1, group_size):
        copy = pltpu.make_async_remote_copy(
            src_ref=mine, dst_ref=got.at[b - 1], send_sem=bs.at[b], recv_sem=br.at[b],
            device_id=along("blk", blk, group_size, b), device_id_type=MESH,
        )
        copy.start()
        far.append(copy)
    best = jnp.max(mine[...], axis=0)
    for b, copy in enumerate(far):
        copy.wait_recv()
        best = jnp.maximum(best, jnp.max(got[b], axis=0))
    out[...] = best
    for copy in copies + far:
        copy.wait_send()


def mlp_kernel(res, peak, shift, up, down, out):
    residual = res[...].reshape(out.shape)
    shifted = node_norm(residual) + shift[...]
    scaled = (4.0 * shifted / (peak[...] + 1e-05)).astype(jnp.bfloat16)
    h = jnp.dot(scaled, up[...], preferred_element_type=jnp.float32)
    h = jax.nn.gelu(h, approximate=True).astype(jnp.bfloat16)
    out[...] = (residual + jnp.dot(h, down[...], preferred_element_type=jnp.float32)).astype(
        jnp.bfloat16
    )


def shards(
    groups, group_size, node_features, norm_gain, norm_shift, query_weight, key_value_weight,
    out_weight, up_weight, down_weight, neighbour_tiles, neighbour_counts,
):
    per_dev = neighbour_tiles.shape[0]
    rows, width = node_features.shape
    tile_rows = rows // per_dev
    pairs = HEADS // 2
    aug = 2 * (width // HEADS) + ONES
    table = per_dev + 8 * CAP
    x = node_features.reshape(per_dev, tile_rows, width)
    gain = norm_gain.reshape(1, width)
    shift = norm_shift.reshape(1, width)
    bf16, f32, i32 = jnp.bfloat16, jnp.float32, jnp.int32
    span = 2 if per_dev % 2 == 0 else 1
    limit = 24 * 1024 * 1024
    keys, vt, qt, flags = pl.pallas_call(
        functools.partial(exchange_kernel, group_size),
        out_shape=(
            jax.ShapeDtypeStruct((table, tile_rows, width), bf16),
            jax.ShapeDtypeStruct((table + 1, pairs, aug, tile_rows), bf16),
            jax.ShapeDtypeStruct((per_dev, width, tile_rows), bf16),
            jax.ShapeDtypeStruct((group_size, 128), i32),
        ),
        in_specs=[SMEM] + [VMEM] * 4,
        out_specs=(VMEM,) * 4,
        scratch_shapes=[
            pltpu.VMEM((group_size, 1, 128), i32),
            pltpu.VMEM((8, 1, 128), i32),
            pltpu.SMEM((8, 1, 128), i32),
            pltpu.VMEM((8, CAP, tile_rows, width), bf16),
            pltpu.VMEM((8, CAP, tile_rows, width), bf16),
            pltpu.SemaphoreType.DMA((8,)),
            pltpu.SemaphoreType.DMA((8,)),
            pltpu.SemaphoreType.DMA((8,)),
            pltpu.SemaphoreType.DMA((8,)),
            pltpu.SemaphoreType.DMA,
        ],
        compiler_params=pltpu.CompilerParams(
            collective_id=0, has_side_effects=True, vmem_limit_bytes=limit
        ),
        name="exchange",
    )(neighbour_tiles, x, gain, query_weight, key_value_weight)
    residual, local_peak = pl.pallas_call(
        functools.partial(attend_kernel, group_size),
        out_shape=(
            jax.ShapeDtypeStruct((per_dev, tile_rows, width), f32),
            jax.ShapeDtypeStruct((1, width), f32),
        ),
        in_specs=[SMEM] * 3 + [VMEM] * 6,
        out_specs=(VMEM,) * 2,
        scratch_shapes=[
            pltpu.SMEM((group_size * per_dev,), i32),
            pltpu.VMEM((width, HEADS * tile_rows), bf16),
            pltpu.VMEM((pairs, aug, 2 * tile_rows), f32),
            pltpu.VMEM((2, 1, 4 * tile_rows), f32),
            pltpu.VMEM((2, 1, 4 * tile_rows), f32),
            pltpu.VMEM((2 * tile_rows, 4 * tile_rows), f32),
            pltpu.VMEM((2 * tile_rows, 4 * tile_rows), f32),
        ],
        compiler_params=pltpu.CompilerParams(vmem_limit_bytes=limit),
        name="attend",
    )(
        neighbour_tiles, neighbour_counts, flags, keys, vt, qt, x, out_weight, shift
    )
    peak = pl.pallas_call(
        functools.partial(peak_kernel, groups, group_size),
        out_shape=jax.ShapeDtypeStruct((1, width), f32),
        in_specs=[VMEM],
        out_specs=VMEM,
        scratch_shapes=[
            pltpu.VMEM((groups, 1, width), f32),
            pltpu.VMEM((group_size - 1, groups, 1, width), f32),
            pltpu.SemaphoreType.DMA,
            pltpu.SemaphoreType.DMA((groups,)),
            pltpu.SemaphoreType.DMA((groups,)),
            pltpu.SemaphoreType.DMA((group_size,)),
            pltpu.SemaphoreType.DMA((group_size,)),
        ],
        compiler_params=pltpu.CompilerParams(collective_id=1, has_side_effects=True),
        name="peak",
    )(local_peak)
    whole = lambda *shape: pl.BlockSpec(shape, lambda i: (0,) * len(shape))
    return pl.pallas_call(
        mlp_kernel,
        grid=(per_dev // span,),
        out_shape=jax.ShapeDtypeStruct((rows, width), bf16),
        in_specs=[
            pl.BlockSpec((span, tile_rows, width), lambda i: (i, 0, 0)),
            whole(1, width),
            whole(1, width),
            whole(*up_weight.shape),
            whole(*down_weight.shape),
        ],
        out_specs=pl.BlockSpec((span * tile_rows, width), lambda i: (i, 0)),
        compiler_params=pltpu.CompilerParams(vmem_limit_bytes=limit),
        name="mlp",
    )(residual, peak, shift, up_weight, down_weight)


def solution(mesh):
    split = P(("grp", "blk"), None)
    body = functools.partial(shards, mesh.shape["grp"], mesh.shape["blk"])
    return jax.shard_map(
        body,
        mesh=mesh,
        in_specs=(split, P(), P(), P(), P(), P(), P(), P(), split, P(("grp", "blk"))),
        out_specs=split,
        check_vma=False,
    )
```
